512 devices in a mesh: tile: 32 (over x, y, core), mem: 16 (over z).
Axes of the slice: x: 4, y: 4, z: 16, core: 2. Of those that a mesh axis runs over, the one named last changes fastest.
Arguments:
- velocity: bfloat16 [96, 2, 8, 131072], P('mem', None, None, 'tile'), may hold values from -6 to 6
- start_frac: float32 [2, 65536], P(None, 'tile'), may hold values from 0 to 1
- observed: float32 [2, 65536], P(None, 'tile'), may hold values from -0.5 to 1.5
- obs_sd: float32 [65536], P('tile'), may hold values from 0.3 to 3
- tile_of: int32 [65536, 1], P('tile'), may hold values from 0 to 31; in each aligned block of 2048 rows (0 to 2047, 2048 to 4095, ...) at most 128 rows name the same one
- cell_of: int32 [65536], P('tile'), may hold values from 0 to 4030, as said below
Outputs:
- analysis_velocity: bfloat16 [96, 2, 8, 131072], P('mem', None, None, 'tile')
- analysis_positions: float32 [96, 2, 65536], P('mem', None, 'tile')
The draws below stay inside these ranges and needn't reach their ends.
Inputs may be any that keep to these rules, and one draw needn't show every extreme that they name: cell_of is i * 64 + j with i and j below 63, so the stencil's four cells lie in the same tile. `tile_of`: of the drifters of one index of tile, at most 128 name one tile, a bound that some block reaches of them.
All inputs are finite; a program needn't handle non-finite values.
Results may differ from the reference program's by a relative error of at most 0.0048.
Values may be sent and summed in bfloat16 or wider, within the bound.
A program may use at most 64 MiB of HBM per device.

```python
import math
import jax
import jax.numpy as jnp
import numpy as np
from jax import lax

MEMBERS = 96
LEVELS = 8
BX = 64
P_DEV = 2048
CELLS = 4096
CELLS_ALL = 131072
DRIFTERS = 65536
CAP = 128
N_TILE = 32


def draw_cell_of(key, part):
    row_index = jax.random.randint(jax.random.fold_in(key, 11), (DRIFTERS,), 0, BX - 1)
    col_index = jax.random.randint(jax.random.fold_in(key, 12), (DRIFTERS,), 0, BX - 1)
    return (row_index * BX + col_index).astype(jnp.int32)


def level_of(stream_key, extent, pieces, low, top_value):
    loudness, own = 1.0, jax.random.fold_in(stream_key, 6)
    for dim, parts in pieces:
        draws = jnp.exp(jax.random.uniform(jax.random.fold_in(own, dim), (parts,), jnp.float32, low / len(pieces), top_value / len(pieces)))
        loudness = loudness * jnp.repeat(draws, extent[dim] // parts).reshape([-1 if axis == dim else 1 for axis in range(len(extent))])
    return loudness


def assign_block(rng, own, number, rows, amount, top, limit, lean):
    sequence = jax.random.permutation(rng, amount)
    heavy_load, ordinary = portions_of(amount, rows * top, limit, lean, True), portions_of(amount, rows * top, limit, lean, False)
    places = jnp.arange(amount)

    def named(lengths, offset_by):
        used = int((lengths > 0).sum())
        fixed = max(1, used // 4)
        moved = fixed + (places - fixed + offset_by * (used - fixed)) % max(1, amount - fixed)
        return jnp.zeros((amount,), jnp.int32).at[sequence[jnp.where(places < fixed, places, moved)]].set(jnp.asarray(lengths, jnp.int32))

    lengths = jnp.where(number % 4 == 0, named(heavy_load, number // 4), named(ordinary, number - number // 4 - 1))
    mixed = jax.random.permutation(jax.random.fold_in(own, 3), amount)
    giver, receiver = mixed[0:amount // 2 * 2:2], mixed[1:amount // 2 * 2:2]
    room = jnp.minimum(lengths[giver] - 1, limit - lengths[receiver]) // 2
    room = jnp.where((giver == sequence[0]) | (receiver == sequence[0]) | (lengths[receiver] == 0), 0, jnp.maximum(room, 0))
    moved = jax.random.randint(jax.random.fold_in(own, 4), (amount // 2,), 0, 1 << 20) % (room + 1)
    lengths = lengths.at[giver].add(-moved).at[receiver].add(moved)
    items = jnp.searchsorted(jnp.cumsum(lengths), jnp.arange(rows * top), side="right").astype(jnp.int32)
    listing = items.reshape(top, rows).T
    listing = listing[jax.random.permutation(jax.random.fold_in(own, 1), rows)]
    offset_by = jax.random.randint(jax.random.fold_in(own, 2), (rows, 1), 0, top)
    return jnp.take_along_axis(listing, (jnp.arange(top)[None, :] + offset_by) % top, axis=1)


def portions_of(number_of, total, reach, skew, full):
    portions = [(1 << 20) // math.isqrt(standing ** skew) + 1 for standing in range(1, number_of + 1)]
    largest = reach if full else min(reach, max(-(-total // number_of), total * portions[0] // sum(portions)))
    least = 1 if total - largest >= number_of - 1 else 0
    holding, surplus = [largest] + [least] * (number_of - 1), total - largest - least * (number_of - 1)
    while surplus > 0:
        candidates = [i for i in range(1, number_of) if holding[i] < largest] or [i for i in range(1, number_of) if holding[i] < reach]
        pool, remaining = sum([portions[i] for i in candidates]), surplus
        for i in candidates:
            extra = min(reach - holding[i], max(1, remaining * portions[i] // pool), surplus)
            holding[i] = holding[i] + extra
            surplus = surplus - extra
    return np.array(holding)


def normal_values(stream_key, extent, width, reach, shards=(), kind=jnp.bfloat16):
    values = jax.random.normal(stream_key, extent, jnp.float32) * width
    if len(shards) > 0:
        values = level_of(stream_key, extent, shards, -0.22, 0.18) * values
    return jnp.clip(values, min=-reach, max=reach).astype(kind)


def setup_inputs(seed: int = 0) -> dict:
    keys = jax.random.split(jax.random.key(seed), 7)
    velocity = normal_values(keys[0], (MEMBERS, 2, LEVELS, CELLS_ALL), 1.0, 6.0, ((0, 16), (3, 32)))
    start_frac = jnp.clip(1.0 * jax.random.uniform(keys[1], (2, DRIFTERS), jnp.float32) ** level_of(keys[1], (2, DRIFTERS), ((1, 32),), -0.2, 0.2), 0.0, 1.0)
    observed = jnp.clip(-0.5 + 2.0 * jax.random.uniform(keys[2], (2, DRIFTERS), jnp.float32) ** level_of(keys[2], (2, DRIFTERS), ((1, 32),), -0.2, 0.2), -0.5, 1.5)
    obs_sd = jnp.clip(jnp.exp(math.log(3.0) - 2.3025851 * jax.random.uniform(keys[3], (DRIFTERS,), jnp.float32) ** level_of(keys[3], (DRIFTERS,), ((0, 32),), -0.2, 0.2)), 0.3, 3.0)
    tile_of_keys = jax.random.split(jax.random.fold_in(keys[4], 1), DRIFTERS // P_DEV)
    tile_of_turns = jax.random.permutation(jax.random.fold_in(keys[4], 3), DRIFTERS // P_DEV)
    tile_of = jax.vmap(lambda own, number: assign_block(jax.random.fold_in(keys[4], 2), own, number, P_DEV, N_TILE, 1, CAP, 2))(tile_of_keys, tile_of_turns).reshape((DRIFTERS, 1))
    cell_of = draw_cell_of(jax.random.fold_in(keys[6], 71), 0)
    return {"velocity": velocity, "start_frac": start_frac, "observed": observed, "obs_sd": obs_sd, "tile_of": tile_of, "cell_of": cell_of}


step_dt = 0.2

def bilinear(corner, position):
    frac_x = position[:, 0:1, :]
    frac_y = position[:, 1:2, :]
    return (1.0 - frac_x) * (1.0 - frac_y) * corner[0] + frac_x * (1.0 - frac_y) * corner[1] + (1.0 - frac_x) * frac_y * corner[2] + frac_x * frac_y * corner[3]

def advect(corner, start):
    position = jnp.broadcast_to(start[None], corner[0].shape)
    for repeat in range(2):
        slope_one = bilinear(corner, position)
        midway = position + 0.5 * step_dt * slope_one
        slope_two = bilinear(corner, midway)
        position = position + step_dt * slope_two
    return position

def ensemble_weights(gram_matrix, projection):
    members = gram_matrix.shape[0]
    identity = jnp.eye(members, dtype=jnp.float32)
    factor = jnp.linalg.cholesky(identity + gram_matrix)
    half_solve = lax.linalg.triangular_solve(factor, projection[:, None], left_side=True, lower=True)
    mean_weight = lax.linalg.triangular_solve(factor, half_solve, left_side=True, lower=True, transpose_a=True)
    inverse_root = lax.linalg.triangular_solve(factor, identity, left_side=True, lower=True, transpose_a=True)
    combined = mean_weight + jnp.sqrt(jnp.float32(members - 1)) * inverse_root
    return combined - lax.optimization_barrier(jnp.mean(combined, axis=0, keepdims=True)) + 1.0 / members

def reference(velocity, start_frac, observed, obs_sd, tile_of, cell_of):
    level_zero = velocity[:, :, 0, :].astype(jnp.float32)
    flat_index = (tile_of[:, 0] * CELLS + cell_of).astype(jnp.int32)
    offsets = (0, 1, BX, BX + 1)
    corner = jnp.stack([jnp.take(level_zero, flat_index + shift_by, axis=2) for shift_by in offsets], 0)
    predicted = advect(corner, start_frac)
    ens_mean = lax.optimization_barrier(jnp.mean(predicted, axis=0))
    inverse_scale = 1.0 / (obs_sd * jnp.sqrt(jnp.float32(MEMBERS - 1)))
    anomaly = ((predicted - ens_mean[None]) * inverse_scale).reshape(MEMBERS, -1)
    innovation = ((observed - ens_mean) / obs_sd).reshape(-1)
    gram_matrix = jnp.dot(anomaly, anomaly.T, precision=lax.Precision.HIGHEST)
    projection = jnp.dot(anomaly, innovation, precision=lax.Precision.HIGHEST)
    weights = ensemble_weights(gram_matrix, projection)
    new_positions = jnp.dot(weights.T, predicted.reshape(MEMBERS, -1), precision=lax.Precision.HIGHEST)
    weights_bf = weights.astype(jnp.bfloat16)
    layers = []
    for component in range(2):
        for level in range(LEVELS):
            layers.append(jnp.dot(weights_bf.T.astype(jnp.float32), velocity[:, component, level, :].astype(jnp.float32), preferred_element_type=jnp.float32).astype(jnp.bfloat16))
    new_velocity = jnp.stack(layers, 1).reshape(MEMBERS, 2, LEVELS, -1)
    return (new_velocity, new_positions.reshape(MEMBERS, 2, -1))
```

```python
import functools

import jax
import jax.numpy as jnp
from jax import lax
from jax.experimental import pallas as pl
from jax.experimental.pallas import tpu as pltpu
from jax.sharding import PartitionSpec as P

BX = 64
LANES = 128
LOW = 256
STEP = 0.2
MESH = pl.DeviceIdType.MESH
HIGHEST = lax.Precision.HIGHEST
BF = jnp.bfloat16
F32 = jnp.float32


def three_parts(x):
    high = x.astype(BF).astype(F32)
    rest = x - high
    middle = rest.astype(BF).astype(F32)
    return high, middle, rest - middle


def nt_dot(a, b, precision=None):
    return lax.dot_general(
        a, b, (((1,), (1,)), ((), ())), precision=precision, preferred_element_type=F32
    )


def bilinear(corner, x, y):
    return (
        (1.0 - x) * (1.0 - y) * corner[0]
        + x * (1.0 - y) * corner[1]
        + (1.0 - x) * y * corner[2]
        + x * y * corner[3]
    )


def remote(src, dst, send_sem, recv_sem, axis, peer):
    return pltpu.make_async_remote_copy(
        src_ref=src,
        dst_ref=dst,
        send_sem=send_sem,
        recv_sem=recv_sem,
        device_id={axis: peer},
        device_id_type=MESH,
    )


def gram_kernel(
    tiles,
    planes,
    local_members,
    dest_ref,
    cell_ref,
    frac_ref,
    obs_ref,
    sd_ref,
    table_ref,
    all_out,
    gram_out,
    slot_ref,
    req,
    asked,
    pred,
    ret,
    parts,
    zsend,
    zall,
    gsend,
    grecv,
    gpart,
    gplane,
    gall,
    send_a,
    send_b,
    send_z,
    recv_a,
    recv_b,
    recv_c,
    recv_e,
):
    me = lax.axis_index("tile")
    mz = lax.axis_index("mem")
    drifters = dest_ref.shape[1]
    width = min(256, drifters)
    members = planes * local_members
    rows = planes * 8

    barrier = pltpu.get_barrier_semaphore()

    def greet_tile(i, carry):
        pl.semaphore_signal(
            barrier, inc=1, device_id={"tile": lax.rem(me + i, tiles)}, device_id_type=MESH
        )
        return carry

    def greet_mem(i, carry):
        pl.semaphore_signal(
            barrier, inc=1, device_id={"mem": lax.rem(mz + i, planes)}, device_id_type=MESH
        )
        return carry

    lax.fori_loop(1, tiles, greet_tile, 0)
    lax.fori_loop(1, planes, greet_mem, 0)

    tile_row = lax.broadcasted_iota(jnp.int32, (tiles, width), 0)
    earlier = (
        lax.broadcasted_iota(jnp.int32, (width, width), 0)
        < lax.broadcasted_iota(jnp.int32, (width, width), 1)
    ).astype(F32).astype(BF)
    count = jnp.zeros((tiles, 1), F32)
    for b in range(drifters // width):
        lanes = pl.ds(b * width, width)
        hot = (tile_row == dest_ref[:, lanes]).astype(F32)
        before = jnp.dot(hot.astype(BF), earlier, preferred_element_type=F32) + count
        slot_ref[:, lanes] = jnp.sum(hot * before, axis=0, keepdims=True)
        count = count + jnp.sum(hot, axis=1, keepdims=True)

    total = jnp.zeros((tiles * 8, LANES), F32)
    for b in range(drifters // width):
        lanes = pl.ds(b * width, width)
        cell = cell_ref[:, lanes]
        values = [(cell >> 8).astype(F32), (cell & (LOW - 1)).astype(F32)]
        values += three_parts(frac_ref[0:1, lanes]) + three_parts(frac_ref[1:2, lanes])
        row = lax.broadcasted_iota(jnp.int32, (8, width), 0)
        block = jnp.broadcast_to(values[7], (8, width))
        for v in range(7):
            block = jnp.where(row == v, values[v], block)
        tile_index = lax.broadcasted_iota(jnp.int32, (tiles, 8, width), 0)
        spread = jnp.where(tile_index == dest_ref[:, lanes][None], block[None], 0.0)
        spread = spread.reshape(tiles * 8, width).astype(BF)
        slot_row = lax.broadcasted_iota(jnp.int32, (LANES, width), 0).astype(F32)
        hot_slot = (slot_row == slot_ref[:, lanes]).astype(F32).astype(BF)
        total = total + nt_dot(spread, hot_slot)
    req[...] = total.reshape(tiles, 8, LANES)

    pl.semaphore_wait(barrier, tiles + planes - 2)

    def ask(i, carry):
        peer = lax.rem(me + i, tiles)
        remote(
            req.at[peer], asked.at[me], send_a.at[peer], recv_a.at[me], "tile", peer
        ).start()
        return carry

    lax.fori_loop(1, tiles, ask, 0)
    asked[me] = req[me]

    def serve(i, carry):
        src = lax.rem(me + tiles - i, tiles)

        @pl.when(i > 0)
        def _():
            remote(
                req.at[src], asked.at[src], send_a.at[src], recv_a.at[src], "tile", src
            ).wait_recv()

        block = asked[src]
        high, low = block[0:1], block[1:2]
        start_x = block[2:3] + block[3:4] + block[4:5]
        start_y = block[5:6] + block[6:7] + block[7:8]
        lows, highs = [], []
        for shift in (0, 1, BX, BX + 1):
            moved = low + float(shift)
            over = moved >= float(LOW)
            lows.append(jnp.where(over, moved - float(LOW), moved))
            highs.append(jnp.where(over, high + 1.0, high))
        low4 = jnp.concatenate(lows, axis=1)
        high4 = jnp.concatenate(highs, axis=1)
        cell_row = lax.broadcasted_iota(jnp.int32, (LOW, 4 * LANES), 0).astype(F32)
        hot = (cell_row == low4).astype(F32).astype(BF)
        found = jnp.dot(table_ref[...], hot, preferred_element_type=F32)
        picked = found[0:16]
        for h in range(1, table_ref.shape[0] // 16):
            picked = jnp.where(high4 == float(h), found[16 * h : 16 * h + 16], picked)
        corner_x = [picked[0:8, LANES * q : LANES * (q + 1)] for q in range(4)]
        corner_y = [picked[8:16, LANES * q : LANES * (q + 1)] for q in range(4)]
        x = jnp.broadcast_to(start_x, (8, LANES))
        y = jnp.broadcast_to(start_y, (8, LANES))
        for _ in range(2):
            half_x = x + 0.5 * STEP * bilinear(corner_x, x, y)
            half_y = y + 0.5 * STEP * bilinear(corner_y, x, y)
            x, y = (
                x + STEP * bilinear(corner_x, half_x, half_y),
                y + STEP * bilinear(corner_y, half_x, half_y),
            )
        pred[src, 0] = x
        pred[src, 1] = y

        @pl.when(i > 0)
        def _():
            remote(
                pred.at[src], ret.at[me], send_b.at[src], recv_b.at[me], "tile", src
            ).start()

        @pl.when(i == 0)
        def _():
            ret[src, 0] = x
            ret[src, 1] = y

        return carry

    lax.fori_loop(0, tiles, serve, 0)

    def asked_sent(i, carry):
        peer = lax.rem(me + i, tiles)
        remote(
            req.at[peer], asked.at[me], send_a.at[peer], recv_a.at[me], "tile", peer
        ).wait_send()
        return carry

    lax.fori_loop(1, tiles, asked_sent, 0)

    def returned(i, carry):
        peer = lax.rem(me + i, tiles)
        copy = remote(pred.at[peer], ret.at[peer], send_b.at[peer], recv_b.at[peer], "tile", peer)
        copy.wait_send()
        copy.wait_recv()
        return carry

    lax.fori_loop(1, tiles, returned, 0)

    for k, part in enumerate(three_parts(ret[...].reshape(tiles * 16, LANES))):
        parts[:, LANES * k : LANES * (k + 1)] = part.astype(BF)
    shares = width // LANES

    def order(i, carry):
        lanes = pl.ds(pl.multiple_of(i * width, width), width)
        slot_row = lax.broadcasted_iota(jnp.int32, (LANES, width), 0).astype(F32)
        hot = (slot_row == slot_ref[:, lanes]).astype(F32).astype(BF)
        hot = jnp.concatenate([hot, hot, hot], axis=0)
        found = jnp.dot(parts[...], hot, preferred_element_type=F32)
        dest = dest_ref[:, lanes]
        picked = found[0:16]
        for t in range(1, tiles):
            picked = jnp.where(dest == t, found[16 * t : 16 * t + 16], picked)
        for s in range(shares):
            zsend[i * shares + s, 0] = picked[0:8, LANES * s : LANES * (s + 1)]
            zsend[i * shares + s, 1] = picked[8:16, LANES * s : LANES * (s + 1)]
        return carry

    lax.fori_loop(0, drifters // width, order, 0)

    def share(i, carry):
        peer = lax.rem(mz + i, planes)
        remote(zsend.at[peer], zall.at[mz], send_z.at[peer], recv_c.at[mz], "mem", peer).start()
        return carry

    lax.fori_loop(1, planes, share, 0)
    zall[mz] = zsend[mz]

    def shared(i, carry):
        peer = lax.rem(mz + i, planes)
        copy = remote(zsend.at[peer], zall.at[peer], send_z.at[peer], recv_c.at[peer], "mem", peer)
        copy.wait_send()
        copy.wait_recv()
        return carry

    lax.fori_loop(1, planes, shared, 0)

    row = lax.broadcasted_iota(jnp.int32, (rows, LANES), 0)
    real = (row & 7) < local_members
    own = pl.ds(pl.multiple_of(mz * LANES, LANES), LANES)
    sd = sd_ref[:, own]
    inverse_scale = 1.0 / (sd * jnp.sqrt(jnp.full(sd.shape, members - 1, F32)))
    gram = jnp.zeros((rows, rows), F32)
    for c in range(2):
        p = zall[:, c].reshape(rows, LANES)
        mean = jnp.sum(jnp.where(real, p, 0.0), axis=0, keepdims=True) * (1.0 / members)
        anomaly = jnp.where(real, (p - mean) * inverse_scale, 0.0)
        innovation = (obs_ref[c : c + 1, own] - mean) / sd
        left = jnp.where(row == local_members, innovation, anomaly)
        gram = gram + nt_dot(left, anomaly, HIGHEST)
    chunk = rows // tiles
    for t in range(tiles):
        gsend[t] = gram[chunk * t : chunk * (t + 1)]

    def scatter(i, carry):
        peer = lax.rem(me + i, tiles)
        remote(gsend.at[peer], grecv.at[me], send_a.at[peer], recv_a.at[me], "tile", peer).start()
        return carry

    lax.fori_loop(1, tiles, scatter, 0)
    grecv[me] = gsend[me]

    def scattered(i, carry):
        peer = lax.rem(me + i, tiles)
        copy = remote(
            gsend.at[peer], grecv.at[peer], send_a.at[peer], recv_a.at[peer], "tile", peer
        )
        copy.wait_send()
        copy.wait_recv()
        return carry

    lax.fori_loop(1, tiles, scattered, 0)
    partial = grecv[0]
    for t in range(1, tiles):
        partial = partial + grecv[t]
    gpart[...] = partial

    def plane(i, carry):
        peer = lax.rem(mz + i, planes)
        remote(gpart, gplane.at[mz], send_z.at[peer], recv_e.at[mz], "mem", peer).start()
        return carry

    lax.fori_loop(1, planes, plane, 0)
    gplane[mz] = partial

    def planed(i, carry):
        peer = lax.rem(mz + i, planes)
        copy = remote(gpart, gplane.at[peer], send_z.at[peer], recv_e.at[peer], "mem", peer)
        copy.wait_send()
        copy.wait_recv()
        return carry

    lax.fori_loop(1, planes, planed, 0)
    summed = gplane[0]
    for z in range(1, planes):
        summed = summed + gplane[z]
    gpart[...] = summed

    def gather(i, carry):
        peer = lax.rem(me + i, tiles)
        remote(gpart, gall.at[me], send_b.at[peer], recv_b.at[me], "tile", peer).start()
        return carry

    lax.fori_loop(1, tiles, gather, 0)
    gall[me] = summed

    def gathered(i, carry):
        peer = lax.rem(me + i, tiles)
        copy = remote(gpart, gall.at[peer], send_b.at[peer], recv_b.at[peer], "tile", peer)
        copy.wait_send()
        copy.wait_recv()
        return carry

    lax.fori_loop(1, tiles, gathered, 0)
    all_out[...] = zall[...]
    gram_out[...] = gall[...]


def gram_of_all(tiles, planes, local_members, dest, cell, frac, obs, sd, table):
    rows = planes * 8
    chunk = rows // tiles
    vmem = pl.BlockSpec(memory_space=pltpu.VMEM)
    dma = pltpu.SemaphoreType.DMA
    f32 = lambda *shape: pltpu.VMEM(shape, F32)
    return pl.pallas_call(
        functools.partial(gram_kernel, tiles, planes, local_members),
        out_shape=(
            jax.ShapeDtypeStruct((planes, 2, 8, LANES), F32),
            jax.ShapeDtypeStruct((tiles, chunk, rows), F32),
        ),
        in_specs=[vmem] * 6,
        out_specs=(vmem, vmem),
        scratch_shapes=[
            f32(1, dest.shape[1]),
            f32(tiles, 8, LANES),
            f32(tiles, 8, LANES),
            f32(tiles, 2, 8, LANES),
            f32(tiles, 2, 8, LANES),
            pltpu.VMEM((tiles * 16, 3 * LANES), BF),
            f32(planes, 2, 8, LANES),
            f32(planes, 2, 8, LANES),
            f32(tiles, chunk, rows),
            f32(tiles, chunk, rows),
            f32(chunk, rows),
            f32(planes, chunk, rows),
            f32(tiles, chunk, rows),
            dma((tiles,)),
            dma((tiles,)),
            dma((planes,)),
            dma((tiles,)),
            dma((tiles,)),
            dma((planes,)),
            dma((planes,)),
        ],
        compiler_params=pltpu.CompilerParams(collective_id=0, has_side_effects=True),
        cost_estimate=pl.CostEstimate(
            flops=100_000_000_000, bytes_accessed=4_000_000, transcendentals=0
        ),
        name="gram",
    )(dest, cell, frac, obs, sd, table)


def combine_kernel(weight_ref, field_ref, *refs):
    out_ref = refs[-1]
    rows = weight_ref.shape[1]
    width = field_ref.shape[2]
    field = field_ref[...].reshape(rows, width)
    out = jnp.dot(weight_ref[...], field, preferred_element_type=F32)
    out_ref[...] = out.astype(BF).reshape(out_ref.shape)


def combine(kron, gathered, first, cells, width, so_far):
    members, layers, part = gathered.shape
    local = kron.shape[0] // layers
    start = first // width
    ins = [
        pl.BlockSpec(kron.shape, lambda i: (0, 0)),
        pl.BlockSpec((members, layers, width), lambda i: (0, 0, i)),
    ]
    args = [kron, gathered]
    alias = {}
    if so_far is not None:
        ins.append(pl.BlockSpec(memory_space=pl.ANY))
        args.append(so_far)
        alias = {2: 0}
    return pl.pallas_call(
        combine_kernel,
        grid=(part // width,),
        in_specs=ins,
        out_specs=pl.BlockSpec((local, layers, width), lambda i: (0, 0, start + i)),
        out_shape=jax.ShapeDtypeStruct((local, layers, cells), BF),
        input_output_aliases=alias,
        cost_estimate=pl.CostEstimate(
            flops=2 * members * local * layers * part,
            bytes_accessed=2 * members * layers * part,
            transcendentals=0,
        ),
        name="combine",
    )(*args)


def ensemble_weights(gram_matrix, projection):
    members = gram_matrix.shape[0]
    identity = jnp.eye(members, dtype=jnp.float32)
    factor = jnp.linalg.cholesky(identity + gram_matrix)
    inverse_root = lax.linalg.triangular_solve(
        factor, identity, left_side=True, lower=True, transpose_a=True
    )
    half_solve = jnp.dot(projection[None], inverse_root, precision=HIGHEST)
    mean_weight = jnp.sum(inverse_root * half_solve, axis=1, keepdims=True)
    combined = mean_weight + jnp.sqrt(jnp.float32(members - 1)) * inverse_root
    return combined - jnp.mean(combined, axis=0, keepdims=True) + 1.0 / members


CHUNKS = (3072, 1024)


def shards(velocity, start_frac, observed, obs_sd, tile_of, cell_of):
    local, comps, levels, cells = velocity.shape
    tiles = lax.axis_size("tile")
    planes = lax.axis_size("mem")
    members = planes * local
    drifters = cell_of.shape[0]
    layers = comps * levels

    field = velocity.reshape(local, layers, cells)
    gathered, first = [], 0
    for size in CHUNKS:
        piece = lax.slice_in_dim(field, first, first + size, axis=2)
        gathered.append((first, lax.all_gather(piece, "mem", axis=0, tiled=True)))
        first += size

    table = velocity[:, :, 0, :].reshape(local, comps, cells // LOW, LOW)
    table = jnp.pad(table.transpose(2, 1, 0, 3), ((0, 0), (0, 0), (0, 8 - local), (0, 0)))
    table = table.reshape(-1, LOW)
    predicted, gram = gram_of_all(
        tiles,
        planes,
        local,
        tile_of.reshape(1, drifters),
        cell_of.reshape(1, drifters),
        start_frac,
        observed,
        obs_sd.reshape(1, drifters),
        table,
    )
    gram = gram.reshape(planes, 8, planes, 8)
    projection = gram[0, local, :, :local].reshape(members)
    gram_matrix = gram[:, :local, :, :local].reshape(members, members)
    weights = ensemble_weights(gram_matrix, projection)

    everyone = predicted[:, :, :local]
    moved = jnp.einsum(
        "zmn,zcmp->ncp", weights.reshape(planes, local, members), everyone, precision=HIGHEST
    )
    moved = lax.all_to_all(
        moved.reshape(planes, local, comps, LANES), "mem", split_axis=0, concat_axis=0, tiled=True
    )
    new_positions = moved.transpose(1, 2, 0, 3).reshape(local, comps, drifters)

    first_member = lax.axis_index("mem") * local
    own_columns = lax.dynamic_slice_in_dim(weights, first_member, local, 1).astype(BF)
    same = jnp.eye(layers, dtype=BF)
    kron = own_columns.T[:, None, :, None] * same[None, :, None, :]
    kron = kron.reshape(local * layers, members * layers)
    out = None
    for first, part in gathered:
        out = combine(kron, part, first, cells, 512, out)
    return (out.reshape(local, comps, levels, cells), new_positions)


def solution(mesh):
    in_specs = (
        P("mem", None, None, "tile"),
        P(None, "tile"),
        P(None, "tile"),
        P("tile"),
        P("tile", None),
        P("tile"),
    )
    out_specs = (P("mem", None, None, "tile"), P("mem", None, "tile"))
    return jax.shard_map(shards, mesh=mesh, in_specs=in_specs, out_specs=out_specs, check_vma=False)
```

```python
import functools

import jax
import jax.numpy as jnp
from jax import lax
from jax.experimental import pallas as pl
from jax.experimental.pallas import tpu as pltpu
from jax.sharding import PartitionSpec as P

BX = 64
LANES = 128
LOW = 256
STEP = 0.2
PLAN = (0, 2, 14, 17, 21, 25, 28, 31, 34, 38, 40)
MESH = pl.DeviceIdType.MESH
HIGHEST = lax.Precision.HIGHEST
BF = jnp.bfloat16
F32 = jnp.float32


def three_parts(x):
    high = x.astype(BF).astype(F32)
    rest = x - high
    middle = rest.astype(BF).astype(F32)
    return high, middle, rest - middle


def nt_dot(a, b, precision=None):
    return lax.dot_general(
        a, b, (((1,), (1,)), ((), ())), precision=precision, preferred_element_type=F32
    )


def bilinear(corner, x, y):
    return (
        (1.0 - x) * (1.0 - y) * corner[0]
        + x * (1.0 - y) * corner[1]
        + (1.0 - x) * y * corner[2]
        + x * y * corner[3]
    )


def remote(src, dst, send_sem, recv_sem, axis, peer):
    return pltpu.make_async_remote_copy(
        src_ref=src,
        dst_ref=dst,
        send_sem=send_sem,
        recv_sem=recv_sem,
        device_id={axis: peer},
        device_id_type=MESH,
    )


PIECES = 8
LEAD = 5


def assimilation_kernel(
    tiles,
    planes,
    local,
    dest_ref,
    cell_ref,
    frac_ref,
    obs_ref,
    sd_ref,
    velocity_ref,
    velocity_out,
    positions_out,
    field,
    table,
    slot_ref,
    req,
    asked,
    pred,
    ret,
    parts,
    zsend,
    zall,
    gsend,
    grecv,
    gpart,
    gplane,
    gall,
    gfull,
    weight_t,
    kron,
    acc,
    psend,
    pall,
    load_sem,
    send_a,
    send_b,
    send_z,
    recv_a,
    recv_b,
    recv_c,
    recv_e,
    recv_g,
    ring_send,
    ring_recv,
):
    me = lax.axis_index("tile")
    mz = lax.axis_index("mem")
    drifters = dest_ref.shape[1]
    width = min(256, drifters)
    members = planes * local
    rows = planes * 8
    layers = velocity_ref.shape[1]
    piece = velocity_ref.shape[2] // PIECES
    inner = local * layers
    reach = planes // 2
    slots = PIECES * (reach - 1) + PIECES // 2

    def own_piece(q):
        return pltpu.make_async_copy(
            velocity_ref.at[:, :, pl.ds(q * piece, piece)], field.at[mz, q], load_sem.at[q]
        )

    for q in range(PIECES):
        own_piece(q).start()

    barrier = pltpu.get_barrier_semaphore()

    def greet_tile(i, carry):
        pl.semaphore_signal(
            barrier, inc=1, device_id={"tile": lax.rem(me + i, tiles)}, device_id_type=MESH
        )
        return carry

    def greet_mem(i, carry):
        pl.semaphore_signal(
            barrier, inc=1, device_id={"mem": lax.rem(mz + i, planes)}, device_id_type=MESH
        )
        return carry

    lax.fori_loop(1, tiles, greet_tile, 0)
    lax.fori_loop(1, planes, greet_mem, 0)
    for q in range(PIECES):
        own_piece(q).wait()
    pl.semaphore_wait(barrier, tiles + planes - 2)

    up = lax.rem(mz + 1, planes)
    down = lax.rem(mz + planes - 1, planes)

    def ring_copy(way, n, source, peer):
        q = lax.rem(n + way * (PIECES // 2), PIECES)
        return remote(
            field.at[source, q],
            field.at[source, q],
            ring_send.at[way, lax.rem(n, PIECES)],
            ring_recv.at[way, n],
            "mem",
            peer,
        )

    def ring_out(way, n):
        back = n // PIECES
        source = lax.rem(mz + planes - back, planes) if way == 0 else lax.rem(mz + back, planes)
        return ring_copy(way, n, source, up if way == 0 else down)

    def ring_source(way, n):
        back = n // PIECES + 1
        return lax.rem(mz + planes - back, planes) if way == 0 else lax.rem(mz + back, planes)

    def ring_in(way, n):
        return ring_copy(way, n, ring_source(way, n), up if way == 0 else down)

    def issue(n):
        for way in range(2):
            ring_out(way, n).start()

    def pump(n):
        for way in range(2):
            ring_in(way, n).wait_recv()
        ahead = n + LEAD

        @pl.when(ahead < slots)
        def _():
            @pl.when(ahead >= PIECES)
            def _():
                for way in range(2):
                    ring_out(way, ahead - PIECES).wait_send()

            issue(ahead)

    def pumps(first, last):
        first, last = min(first, slots - 4), min(last, slots - 4)
        if last > first:

            def one(n, carry):
                pump(n)
                return carry

            lax.fori_loop(first, last, one, 0)

    def pumps_in_loop(first, last, i, steps):
        first, last = min(first, slots - 4), min(last, slots - 4)
        count = last - first
        if count > 0:

            def one(n, carry):
                pump(n)
                return carry

            lax.fori_loop(first + i * count // steps, first + (i + 1) * count // steps, one, 0)

    for n in range(min(LEAD, slots)):
        issue(n)

    pick_row = lax.broadcasted_iota(jnp.int32, (16, inner), 0)
    pick_column = lax.broadcasted_iota(jnp.int32, (16, inner), 1)
    half = layers // 2
    pick = ((pick_column // layers) == (pick_row & 7)) & (
        (pick_column % layers) == half * (pick_row >> 3)
    )
    pick = pick.astype(F32).astype(BF)
    for q in range(PIECES):
        level = jnp.dot(
            pick, field[mz, q].reshape(inner, piece), preferred_element_type=F32
        ).astype(BF)
        for h in range(piece // LOW):
            first = (q * (piece // LOW) + h) * 16
            table[first : first + 16, :] = level[:, LOW * h : LOW * (h + 1)]

    tile_row = lax.broadcasted_iota(jnp.int32, (tiles, width), 0)
    earlier = (
        lax.broadcasted_iota(jnp.int32, (width, width), 0)
        < lax.broadcasted_iota(jnp.int32, (width, width), 1)
    ).astype(F32).astype(BF)
    count = jnp.zeros((tiles, 1), F32)
    for b in range(drifters // width):
        lanes = pl.ds(b * width, width)
        hot = (tile_row == dest_ref[:, lanes]).astype(F32)
        before = jnp.dot(hot.astype(BF), earlier, preferred_element_type=F32) + count
        slot_ref[:, lanes] = jnp.sum(hot * before, axis=0, keepdims=True)
        count = count + jnp.sum(hot, axis=1, keepdims=True)

    total = jnp.zeros((tiles * 8, LANES), F32)
    for b in range(drifters // width):
        lanes = pl.ds(b * width, width)
        cell = cell_ref[:, lanes]
        values = [(cell >> 8).astype(F32), (cell & (LOW - 1)).astype(F32)]
        values += three_parts(frac_ref[0:1, lanes]) + three_parts(frac_ref[1:2, lanes])
        row = lax.broadcasted_iota(jnp.int32, (8, width), 0)
        block = jnp.broadcast_to(values[7], (8, width))
        for v in range(7):
            block = jnp.where(row == v, values[v], block)
        tile_index = lax.broadcasted_iota(jnp.int32, (tiles, 8, width), 0)
        spread = jnp.where(tile_index == dest_ref[:, lanes][None], block[None], 0.0)
        spread = spread.reshape(tiles * 8, width).astype(BF)
        slot_row = lax.broadcasted_iota(jnp.int32, (LANES, width), 0).astype(F32)
        hot_slot = (slot_row == slot_ref[:, lanes]).astype(F32).astype(BF)
        total = total + nt_dot(spread, hot_slot)
    req[...] = total.reshape(tiles, 8, LANES)

    def ask(i, carry):
        peer = lax.rem(me + i, tiles)
        remote(
            req.at[peer], asked.at[me], send_a.at[peer], recv_a.at[me], "tile", peer
        ).start()
        return carry

    lax.fori_loop(1, tiles, ask, 0)
    asked[me] = req[me]

    pumps(PLAN[0], PLAN[1])

    def serve(i, carry):
        src = lax.rem(me + tiles - i, tiles)

        @pl.when(i > 0)
        def _():
            remote(
                req.at[src], asked.at[src], send_a.at[src], recv_a.at[src], "tile", src
            ).wait_recv()

        block = asked[src]
        high, low = block[0:1], block[1:2]
        start_x = block[2:3] + block[3:4] + block[4:5]
        start_y = block[5:6] + block[6:7] + block[7:8]
        lows, highs = [], []
        for shift in (0, 1, BX, BX + 1):
            moved = low + float(shift)
            over = moved >= float(LOW)
            lows.append(jnp.where(over, moved - float(LOW), moved))
            highs.append(jnp.where(over, high + 1.0, high))
        low4 = jnp.concatenate(lows, axis=1)
        high4 = jnp.concatenate(highs, axis=1)
        cell_row = lax.broadcasted_iota(jnp.int32, (LOW, 4 * LANES), 0).astype(F32)
        hot = (cell_row == low4).astype(F32).astype(BF)
        found = jnp.dot(table[...], hot, preferred_element_type=F32)
        picked = found[0:16]
        for h in range(1, table.shape[0] // 16):
            picked = jnp.where(high4 == float(h), found[16 * h : 16 * h + 16], picked)
        corner_x = [picked[0:8, LANES * q : LANES * (q + 1)] for q in range(4)]
        corner_y = [picked[8:16, LANES * q : LANES * (q + 1)] for q in range(4)]
        x = jnp.broadcast_to(start_x, (8, LANES))
        y = jnp.broadcast_to(start_y, (8, LANES))
        for _ in range(2):
            half_x = x + 0.5 * STEP * bilinear(corner_x, x, y)
            half_y = y + 0.5 * STEP * bilinear(corner_y, x, y)
            x, y = (
                x + STEP * bilinear(corner_x, half_x, half_y),
                y + STEP * bilinear(corner_y, half_x, half_y),
            )
        pred[src, 0] = x
        pred[src, 1] = y

        @pl.when(i > 0)
        def _():
            remote(
                pred.at[src], ret.at[me], send_b.at[src], recv_b.at[me], "tile", src
            ).start()

        @pl.when(i == 0)
        def _():
            ret[src, 0] = x
            ret[src, 1] = y

        pumps_in_loop(PLAN[1], PLAN[2], i, tiles)

        return carry

    lax.fori_loop(0, tiles, serve, 0)

    def asked_sent(i, carry):
        peer = lax.rem(me + i, tiles)
        remote(
            req.at[peer], asked.at[me], send_a.at[peer], recv_a.at[me], "tile", peer
        ).wait_send()
        return carry

    lax.fori_loop(1, tiles, asked_sent, 0)

    pumps(PLAN[2], PLAN[3])

    def returned(i, carry):
        peer = lax.rem(me + i, tiles)
        copy = remote(pred.at[peer], ret.at[peer], send_b.at[peer], recv_b.at[peer], "tile", peer)
        copy.wait_send()
        copy.wait_recv()
        return carry

    lax.fori_loop(1, tiles, returned, 0)

    for k, part in enumerate(three_parts(ret[...].reshape(tiles * 16, LANES))):
        parts[:, LANES * k : LANES * (k + 1)] = part.astype(BF)
    shares = width // LANES

    def order(i, carry):
        lanes = pl.ds(pl.multiple_of(i * width, width), width)
        slot_row = lax.broadcasted_iota(jnp.int32, (LANES, width), 0).astype(F32)
        hot = (slot_row == slot_ref[:, lanes]).astype(F32).astype(BF)
        hot = jnp.concatenate([hot, hot, hot], axis=0)
        found = jnp.dot(parts[...], hot, preferred_element_type=F32)
        dest = dest_ref[:, lanes]
        picked = found[0:16]
        for t in range(1, tiles):
            picked = jnp.where(dest == t, found[16 * t : 16 * t + 16], picked)
        for s in range(shares):
            zsend[i * shares + s, 0] = picked[0:8, LANES * s : LANES * (s + 1)]
            zsend[i * shares + s, 1] = picked[8:16, LANES * s : LANES * (s + 1)]
        pumps_in_loop(PLAN[3], PLAN[4], i, drifters // width)
        return carry

    lax.fori_loop(0, drifters // width, order, 0)

    def share(i, carry):
        peer = lax.rem(mz + i, planes)
        remote(zsend.at[peer], zall.at[mz], send_z.at[peer], recv_c.at[mz], "mem", peer).start()
        return carry

    lax.fori_loop(1, planes, share, 0)
    zall[mz] = zsend[mz]
    pumps(PLAN[4], PLAN[5])

    def shared(i, carry):
        peer = lax.rem(mz + i, planes)
        copy = remote(zsend.at[peer], zall.at[peer], send_z.at[peer], recv_c.at[peer], "mem", peer)
        copy.wait_send()
        copy.wait_recv()
        return carry

    lax.fori_loop(1, planes, shared, 0)

    row = lax.broadcasted_iota(jnp.int32, (rows, LANES), 0)
    real = (row & 7) < local
    own = pl.ds(pl.multiple_of(mz * LANES, LANES), LANES)
    sd = sd_ref[:, own]
    inverse_scale = 1.0 / (sd * jnp.sqrt(jnp.full(sd.shape, members - 1, F32)))
    gram = jnp.zeros((rows, rows), F32)
    for c in range(2):
        p = zall[:, c].reshape(rows, LANES)
        mean = jnp.sum(jnp.where(real, p, 0.0), axis=0, keepdims=True) * (1.0 / members)
        anomaly = jnp.where(real, (p - mean) * inverse_scale, 0.0)
        innovation = (obs_ref[c : c + 1, own] - mean) / sd
        left = jnp.where(row == local, innovation, anomaly)
        gram = gram + nt_dot(left, anomaly, HIGHEST)
    chunk = rows // tiles
    for t in range(tiles):
        gsend[t] = gram[chunk * t : chunk * (t + 1)]

    def scatter(i, carry):
        peer = lax.rem(me + i, tiles)
        remote(gsend.at[peer], grecv.at[me], send_a.at[peer], recv_a.at[me], "tile", peer).start()
        return carry

    lax.fori_loop(1, tiles, scatter, 0)
    grecv[me] = gsend[me]
    pumps(PLAN[5], PLAN[6])

    def scattered(i, carry):
        peer = lax.rem(me + i, tiles)
        copy = remote(
            gsend.at[peer], grecv.at[peer], send_a.at[peer], recv_a.at[peer], "tile", peer
        )
        copy.wait_send()
        copy.wait_recv()
        return carry

    lax.fori_loop(1, tiles, scattered, 0)
    partial = grecv[0]
    for t in range(1, tiles):
        partial = partial + grecv[t]
    gpart[...] = partial

    def plane(i, carry):
        peer = lax.rem(mz + i, planes)
        remote(gpart, gplane.at[mz], send_z.at[peer], recv_e.at[mz], "mem", peer).start()
        return carry

    lax.fori_loop(1, planes, plane, 0)
    gplane[mz] = partial
    pumps(PLAN[6], PLAN[7])

    def planed(i, carry):
        peer = lax.rem(mz + i, planes)
        copy = remote(gpart, gplane.at[peer], send_z.at[peer], recv_e.at[peer], "mem", peer)
        copy.wait_send()
        copy.wait_recv()
        return carry

    lax.fori_loop(1, planes, planed, 0)
    summed = gplane[0]
    for z in range(1, planes):
        summed = summed + gplane[z]
    gpart[...] = summed

    def gather(i, carry):
        peer = lax.rem(me + i, tiles)
        remote(gpart, gall.at[me], send_b.at[peer], recv_b.at[me], "tile", peer).start()
        return carry

    lax.fori_loop(1, tiles, gather, 0)
    gall[me] = summed
    pumps(PLAN[7], PLAN[8])

    def gathered(i, carry):
        peer = lax.rem(me + i, tiles)
        copy = remote(gpart, gall.at[peer], send_b.at[peer], recv_b.at[peer], "tile", peer)
        copy.wait_send()
        copy.wait_recv()
        return carry

    lax.fori_loop(1, tiles, gathered, 0)

    for t in range(tiles):
        gfull[chunk * t : chunk * (t + 1), :] = gall[t]
    proj_row = gfull[local : local + 1, :]
    square_row = lax.broadcasted_iota(jnp.int32, (rows, rows), 0)
    square_column = lax.broadcasted_iota(jnp.int32, (rows, rows), 1)
    one = (square_row == square_column).astype(F32)
    left = jnp.where((square_row & 7) < local, gfull[...], 0.0) + one
    inverse = one
    for b in range(planes):
        height = rows - 8 * b
        step_row = lax.broadcasted_iota(jnp.int32, (height, rows), 0)
        for r in range(local):
            k = 8 * b + r
            pivot = left[r : r + 1, k : k + 1]
            scale = lax.rsqrt(pivot)
            scale = scale * (1.5 - 0.5 * pivot * scale * scale)
            left_row = left[r : r + 1] * scale
            inverse_row = inverse[r : r + 1] * scale
            column = jnp.where(step_row > r, left[:, k : k + 1] * scale, 0.0)
            left = left - column * left_row
            inverse = jnp.where(step_row == r, inverse_row, inverse - column * inverse_row)
        weight_t[8 * b : 8 * b + 8, :] = inverse[0:8]
        if b + 1 < planes:
            left, inverse = left[8:], inverse[8:]
        pumps(PLAN[8] + (PLAN[9] - PLAN[8]) * b // planes, PLAN[8] + (PLAN[9] - PLAN[8]) * (b + 1) // planes)

    real_square = ((square_row & 7) < local) & ((square_column & 7) < local)
    root = jnp.where(real_square, weight_t[...], 0.0)
    solved = jnp.sum(root * proj_row, axis=1, keepdims=True)
    mean_weight = jnp.sum(root * solved, axis=0, keepdims=True)
    grown = mean_weight + jnp.sqrt(jnp.full((rows, rows), members - 1, F32)) * root
    grown = jnp.where(real_square, grown, 0.0)
    centre = jnp.sum(grown, axis=1, keepdims=True) * (1.0 / members)
    weights = jnp.where(real_square, grown - centre + 1.0 / members, 0.0)
    weight_t[...] = weights

    for c in range(2):
        share_of = zall[:, c].reshape(rows, LANES)
        share_of = jnp.where(real, share_of, 0.0)
        moved = jnp.dot(weights, share_of, precision=HIGHEST, preferred_element_type=F32)
        psend[:, c] = moved.reshape(planes, 8, LANES)

    def give(i, carry):
        peer = lax.rem(mz + i, planes)
        remote(psend.at[peer], pall.at[mz], send_z.at[peer], recv_g.at[mz], "mem", peer).start()
        return carry

    lax.fori_loop(1, planes, give, 0)
    pall[mz] = psend[mz]
    pumps(PLAN[9], PLAN[10])

    own_weights = weight_t[pl.ds(pl.multiple_of(mz * 8, 8), 8), :].astype(BF)
    up_row = lax.broadcasted_iota(jnp.int32, (inner, 8), 0)
    up_column = lax.broadcasted_iota(jnp.int32, (inner, 8), 1)
    tall = jnp.dot(
        ((up_row // layers) == up_column).astype(F32).astype(BF),
        own_weights,
        preferred_element_type=F32,
    ).astype(BF)
    for z in range(planes):
        wide_row = lax.broadcasted_iota(jnp.int32, (rows, 8 * layers), 0)
        wide_column = lax.broadcasted_iota(jnp.int32, (rows, 8 * layers), 1)
        spread = jnp.dot(
            tall,
            (wide_row == 8 * z + wide_column // layers).astype(F32).astype(BF),
            preferred_element_type=F32,
        )
        same = (lax.broadcasted_iota(jnp.int32, (inner, 8 * layers), 0) % layers) == (
            lax.broadcasted_iota(jnp.int32, (inner, 8 * layers), 1) % layers
        )
        kron[z] = jnp.where(same, spread, 0.0).astype(BF)

    def term(source, q):
        block = field[source, q].reshape(inner, piece)
        return jnp.dot(kron[source][:, :inner], block, preferred_element_type=F32)

    def own_term(q, carry):
        acc[q] = term(mz, q)
        return carry

    lax.fori_loop(0, PIECES, own_term, 0)

    def add_slot(n):
        for way in range(2):
            q = lax.rem(n + way * (PIECES // 2), PIECES)
            acc[q] = acc[q] + term(ring_source(way, n), q)

    begin = min(PLAN[10], slots - 4)
    rest = slots - begin - 2

    def follow(n, carry):
        pump(n)
        j = n - begin

        def late(s, carry):
            add_slot(s)
            return carry

        lax.fori_loop(
            jnp.minimum(j * begin // rest, begin), jnp.minimum((j + 1) * begin // rest, begin), late, 0
        )
        add_slot(n)
        return carry

    lax.fori_loop(begin, slots, follow, 0)
    for q in range(PIECES):
        velocity_out[:, :, piece * q : piece * (q + 1)] = (
            acc[q].astype(BF).reshape(local, layers, piece)
        )

    def given(i, carry):
        peer = lax.rem(mz + i, planes)
        copy = remote(psend.at[peer], pall.at[peer], send_z.at[peer], recv_g.at[peer], "mem", peer)
        copy.wait_send()
        copy.wait_recv()
        return carry

    lax.fori_loop(1, planes, given, 0)

    def place(z, carry):
        lanes = pl.ds(pl.multiple_of(z * LANES, LANES), LANES)
        for c in range(2):
            block = pall[z, c]
            for m in range(local):
                positions_out[m, c : c + 1, lanes] = block[m : m + 1]
        return carry

    lax.fori_loop(0, planes, place, 0)
    for n in range(max(slots - PIECES, 0), slots):
        for way in range(2):
            ring_out(way, n).wait_send()


def shards(velocity, start_frac, observed, obs_sd, tile_of, cell_of):
    local, comps, levels, cells = velocity.shape
    tiles = lax.axis_size("tile")
    planes = lax.axis_size("mem")
    drifters = cell_of.shape[0]
    layers = comps * levels
    rows = planes * 8
    chunk = rows // tiles
    inner = local * layers
    piece = cells // PIECES
    slots = PIECES * (planes // 2 - 1) + PIECES // 2
    vmem = pl.BlockSpec(memory_space=pltpu.VMEM)
    dma = pltpu.SemaphoreType.DMA
    f32 = lambda *shape: pltpu.VMEM(shape, F32)
    bf16 = lambda *shape: pltpu.VMEM(shape, BF)
    new_velocity, new_positions = pl.pallas_call(
        functools.partial(assimilation_kernel, tiles, planes, local),
        out_shape=(
            jax.ShapeDtypeStruct((local, layers, cells), BF),
            jax.ShapeDtypeStruct((local, comps, drifters), F32),
        ),
        in_specs=[vmem] * 5 + [pl.BlockSpec(memory_space=pl.ANY)],
        out_specs=(vmem, vmem),
        scratch_shapes=[
            bf16(planes, PIECES, local, layers, piece),
            bf16(cells // LOW * 16, LOW),
            f32(1, drifters),
            f32(tiles, 8, LANES),
            f32(tiles, 8, LANES),
            f32(tiles, 2, 8, LANES),
            f32(tiles, 2, 8, LANES),
            bf16(tiles * 16, 3 * LANES),
            f32(planes, 2, 8, LANES),
            f32(planes, 2, 8, LANES),
            f32(tiles, chunk, rows),
            f32(tiles, chunk, rows),
            f32(chunk, rows),
            f32(planes, chunk, rows),
            f32(tiles, chunk, rows),
            f32(rows, rows),
            f32(rows, rows),
            bf16(planes, inner, 8 * layers),
            f32(PIECES, inner, piece),
            f32(planes, 2, 8, LANES),
            f32(planes, 2, 8, LANES),
            dma((PIECES,)),
            dma((tiles,)),
            dma((tiles,)),
            dma((planes,)),
            dma((tiles,)),
            dma((tiles,)),
            dma((planes,)),
            dma((planes,)),
            dma((planes,)),
            dma((2, PIECES)),
            dma((2, slots)),
        ],
        compiler_params=pltpu.CompilerParams(
            collective_id=0, has_side_effects=True, vmem_limit_bytes=56 << 20
        ),
        name="assimilation",
    )(
        tile_of.reshape(1, drifters),
        cell_of.reshape(1, drifters),
        start_frac,
        observed,
        obs_sd.reshape(1, drifters),
        velocity.reshape(local, layers, cells),
    )
    return (new_velocity.reshape(velocity.shape), new_positions)


def solution(mesh):
    in_specs = (
        P("mem", None, None, "tile"),
        P(None, "tile"),
        P(None, "tile"),
        P("tile"),
        P("tile", None),
        P("tile"),
    )
    out_specs = (P("mem", None, None, "tile"), P("mem", None, "tile"))
    return jax.shard_map(shards, mesh=mesh, in_specs=in_specs, out_specs=out_specs, check_vma=False)
```

```python
import functools

import jax
import jax.numpy as jnp
from jax import lax
from jax.experimental import pallas as pl
from jax.experimental.pallas import tpu as pltpu
from jax.sharding import PartitionSpec as P

BX = 64
LANES = 128
LOW = 256
STEP = 0.2
PLAN = (0, 2, 14, 17, 21, 25, 28, 31, 34, 38, 40)
MESH = pl.DeviceIdType.MESH
HIGHEST = lax.Precision.HIGHEST
BF = jnp.bfloat16
F32 = jnp.float32


def three_parts(x):
    high = x.astype(BF).astype(F32)
    rest = x - high
    middle = rest.astype(BF).astype(F32)
    return high, middle, rest - middle


def nt_dot(a, b, precision=None):
    return lax.dot_general(
        a, b, (((1,), (1,)), ((), ())), precision=precision, preferred_element_type=F32
    )


def bilinear(corner, x, y):
    return (
        (1.0 - x) * (1.0 - y) * corner[0]
        + x * (1.0 - y) * corner[1]
        + (1.0 - x) * y * corner[2]
        + x * y * corner[3]
    )


def remote(src, dst, send_sem, recv_sem, axis, peer):
    return pltpu.make_async_remote_copy(
        src_ref=src,
        dst_ref=dst,
        send_sem=send_sem,
        recv_sem=recv_sem,
        device_id={axis: peer},
        device_id_type=MESH,
    )


PIECES = 8
LEAD = 5
UP = 4


def assimilation_kernel(
    tiles,
    planes,
    local,
    dest_ref,
    cell_ref,
    frac_ref,
    obs_ref,
    sd_ref,
    velocity_ref,
    velocity_out,
    positions_out,
    field,
    table,
    slot_ref,
    req,
    asked,
    pred,
    ret,
    parts,
    zsend,
    zall,
    zpad,
    gsend,
    grecv,
    gpart,
    gplane,
    gall,
    gfull,
    weight_t,
    kron,
    acc,
    pstage,
    psend,
    pall,
    load_sem,
    send_a,
    send_b,
    send_z,
    recv_a,
    recv_b,
    recv_c,
    recv_e,
    recv_g,
    ring_send,
    ring_recv,
):
    me = lax.axis_index("tile")
    mz = lax.axis_index("mem")
    drifters = dest_ref.shape[1]
    width = min(256, drifters)
    members = planes * local
    rows = planes * 8
    layers = velocity_ref.shape[1]
    piece = velocity_ref.shape[2] // PIECES
    inner = local * layers
    reach = planes // 2
    base = PIECES * (reach - 1)
    slots = (base + UP, base + PIECES - UP)
    shift = (0, UP)

    def own_piece(q):
        return pltpu.make_async_copy(
            velocity_ref.at[:, :, pl.ds(q * piece, piece)], field.at[mz, q], load_sem.at[q]
        )

    for q in range(PIECES):
        own_piece(q).start()

    up = lax.rem(mz + 1, planes)
    down = lax.rem(mz + planes - 1, planes)
    barrier = pltpu.get_barrier_semaphore()

    def greet_tile(i, carry):
        pl.semaphore_signal(
            barrier, inc=1, device_id={"tile": lax.rem(me + i, tiles)}, device_id_type=MESH
        )
        return carry

    lax.fori_loop(1, tiles, greet_tile, 0)

    def greet_mem(i, carry):
        pl.semaphore_signal(
            barrier, inc=1, device_id={"mem": lax.rem(mz + i, planes)}, device_id_type=MESH
        )
        return carry

    lax.fori_loop(1, planes, greet_mem, 0)
    for q in range(PIECES):
        own_piece(q).wait()
    pl.semaphore_wait(barrier, tiles + planes - 2)

    def ring_copy(way, n, source, peer):
        q = lax.rem(n + shift[way], PIECES)
        return remote(
            field.at[source, q],
            field.at[source, q],
            ring_send.at[way, lax.rem(n, PIECES)],
            ring_recv.at[way, n],
            "mem",
            peer,
        )

    def ring_out(way, n):
        back = n // PIECES
        source = lax.rem(mz + planes - back, planes) if way == 0 else lax.rem(mz + back, planes)
        return ring_copy(way, n, source, up if way == 0 else down)

    def ring_source(way, n):
        back = n // PIECES + 1
        return lax.rem(mz + planes - back, planes) if way == 0 else lax.rem(mz + back, planes)

    def ring_in(way, n):
        return ring_copy(way, n, ring_source(way, n), up if way == 0 else down)

    def pump(n, ways=(0, 1)):
        ahead = n + LEAD
        for way in ways:
            ring_in(way, n).wait_recv()

            @pl.when(ahead < slots[way])
            def _():
                @pl.when(ahead >= PIECES)
                def _():
                    ring_out(way, ahead - PIECES).wait_send()

                ring_out(way, ahead).start()

    def pumps(first, last):
        first, last = min(first, base - 4), min(last, base - 4)
        if last > first:

            def one(n, carry):
                pump(n)
                return carry

            lax.fori_loop(first, last, one, 0)

    def pumps_in_loop(first, last, i, steps):
        first, last = min(first, base - 4), min(last, base - 4)
        count = last - first
        if count > 0:

            def one(n, carry):
                pump(n)
                return carry

            lax.fori_loop(first + i * count // steps, first + (i + 1) * count // steps, one, 0)

    for n in range(LEAD):
        for way in range(2):
            ring_out(way, n).start()

    pick_row = lax.broadcasted_iota(jnp.int32, (16, inner), 0)
    pick_column = lax.broadcasted_iota(jnp.int32, (16, inner), 1)
    half = layers // 2
    pick = ((pick_column // layers) == (pick_row & 7)) & (
        (pick_column % layers) == half * (pick_row >> 3)
    )
    pick = pick.astype(F32).astype(BF)
    for q in range(PIECES):
        level = jnp.dot(
            pick, field[mz, q].reshape(inner, piece), preferred_element_type=F32
        ).astype(BF)
        for h in range(piece // LOW):
            first = (q * (piece // LOW) + h) * 16
            table[first : first + 16, :] = level[:, LOW * h : LOW * (h + 1)]

    tile_row = lax.broadcasted_iota(jnp.int32, (tiles, width), 0)
    earlier = (
        lax.broadcasted_iota(jnp.int32, (width, width), 0)
        < lax.broadcasted_iota(jnp.int32, (width, width), 1)
    ).astype(F32).astype(BF)
    count = jnp.zeros((tiles, 1), F32)
    for b in range(drifters // width):
        lanes = pl.ds(b * width, width)
        hot = (tile_row == dest_ref[:, lanes]).astype(F32)
        before = jnp.dot(hot.astype(BF), earlier, preferred_element_type=F32) + count
        slot_ref[:, lanes] = jnp.sum(hot * before, axis=0, keepdims=True)
        count = count + jnp.sum(hot, axis=1, keepdims=True)

    total = jnp.zeros((tiles * 8, LANES), F32)
    for b in range(drifters // width):
        lanes = pl.ds(b * width, width)
        cell = cell_ref[:, lanes]
        values = [(cell >> 8).astype(F32), (cell & (LOW - 1)).astype(F32)]
        values += three_parts(frac_ref[0:1, lanes]) + three_parts(frac_ref[1:2, lanes])
        row = lax.broadcasted_iota(jnp.int32, (8, width), 0)
        block = jnp.broadcast_to(values[7], (8, width))
        for v in range(7):
            block = jnp.where(row == v, values[v], block)
        tile_index = lax.broadcasted_iota(jnp.int32, (tiles, 8, width), 0)
        spread = jnp.where(tile_index == dest_ref[:, lanes][None], block[None], 0.0)
        spread = spread.reshape(tiles * 8, width).astype(BF)
        slot_row = lax.broadcasted_iota(jnp.int32, (LANES, width), 0).astype(F32)
        hot_slot = (slot_row == slot_ref[:, lanes]).astype(F32).astype(BF)
        total = total + nt_dot(spread, hot_slot)
    req[...] = total.reshape(tiles, 8, LANES)

    def ask(i, carry):
        peer = lax.rem(me + i, tiles)
        remote(
            req.at[peer], asked.at[me], send_a.at[peer], recv_a.at[me], "tile", peer
        ).start()
        return carry

    lax.fori_loop(1, tiles, ask, 0)
    asked[me] = req[me]

    pumps(PLAN[0], PLAN[1])

    def serve(i, carry):
        src = lax.rem(me + tiles - i, tiles)

        @pl.when(i > 0)
        def _():
            remote(
                req.at[src], asked.at[src], send_a.at[src], recv_a.at[src], "tile", src
            ).wait_recv()

        block = asked[src]
        high, low = block[0:1], block[1:2]
        start_x = block[2:3] + block[3:4] + block[4:5]
        start_y = block[5:6] + block[6:7] + block[7:8]
        lows, highs = [], []
        for shift in (0, 1, BX, BX + 1):
            moved = low + float(shift)
            over = moved >= float(LOW)
            lows.append(jnp.where(over, moved - float(LOW), moved))
            highs.append(jnp.where(over, high + 1.0, high))
        low4 = jnp.concatenate(lows, axis=1)
        high4 = jnp.concatenate(highs, axis=1)
        cell_row = lax.broadcasted_iota(jnp.int32, (LOW, 4 * LANES), 0).astype(F32)
        hot = (cell_row == low4).astype(F32).astype(BF)
        found = jnp.dot(table[...], hot, preferred_element_type=F32)
        picked = found[0:16]
        for h in range(1, table.shape[0] // 16):
            picked = jnp.where(high4 == float(h), found[16 * h : 16 * h + 16], picked)
        corner_x = [picked[0:8, LANES * q : LANES * (q + 1)] for q in range(4)]
        corner_y = [picked[8:16, LANES * q : LANES * (q + 1)] for q in range(4)]
        x = jnp.broadcast_to(start_x, (8, LANES))
        y = jnp.broadcast_to(start_y, (8, LANES))
        for _ in range(2):
            half_x = x + 0.5 * STEP * bilinear(corner_x, x, y)
            half_y = y + 0.5 * STEP * bilinear(corner_y, x, y)
            x, y = (
                x + STEP * bilinear(corner_x, half_x, half_y),
                y + STEP * bilinear(corner_y, half_x, half_y),
            )
        pred[src, 0] = x
        pred[src, 1] = y

        @pl.when(i > 0)
        def _():
            remote(
                pred.at[src], ret.at[me], send_b.at[src], recv_b.at[me], "tile", src
            ).start()

        @pl.when(i == 0)
        def _():
            ret[src, 0] = x
            ret[src, 1] = y

        pumps_in_loop(PLAN[1], PLAN[2], i, tiles)

        return carry

    lax.fori_loop(0, tiles, serve, 0)

    def asked_sent(i, carry):
        peer = lax.rem(me + i, tiles)
        remote(
            req.at[peer], asked.at[me], send_a.at[peer], recv_a.at[me], "tile", peer
        ).wait_send()
        return carry

    lax.fori_loop(1, tiles, asked_sent, 0)

    pumps(PLAN[2], PLAN[3])

    def returned(i, carry):
        peer = lax.rem(me + i, tiles)
        copy = remote(pred.at[peer], ret.at[peer], send_b.at[peer], recv_b.at[peer], "tile", peer)
        copy.wait_send()
        copy.wait_recv()
        return carry

    lax.fori_loop(1, tiles, returned, 0)

    for k, part in enumerate(three_parts(ret[...].reshape(tiles * 16, LANES))):
        parts[:, LANES * k : LANES * (k + 1)] = part.astype(BF)
    shares = width // LANES

    def order(i, carry):
        lanes = pl.ds(pl.multiple_of(i * width, width), width)
        slot_row = lax.broadcasted_iota(jnp.int32, (LANES, width), 0).astype(F32)
        hot = (slot_row == slot_ref[:, lanes]).astype(F32).astype(BF)
        hot = jnp.concatenate([hot, hot, hot], axis=0)
        found = jnp.dot(parts[...], hot, preferred_element_type=F32)
        dest = dest_ref[:, lanes]
        picked = found[0:16]
        for t in range(1, tiles):
            picked = jnp.where(dest == t, found[16 * t : 16 * t + 16], picked)
        for s in range(shares):
            lanes_of = slice(LANES * s, LANES * (s + 1))
            zsend[i * shares + s, 0:local] = picked[0:local, lanes_of]
            zsend[i * shares + s, local : 2 * local] = picked[8 : 8 + local, lanes_of]
        pumps_in_loop(PLAN[3], PLAN[4], i, drifters // width)
        return carry

    lax.fori_loop(0, drifters // width, order, 0)

    def share(i, carry):
        peer = lax.rem(mz + i, planes)
        remote(zsend.at[peer], zall.at[mz], send_z.at[peer], recv_c.at[mz], "mem", peer).start()
        return carry

    lax.fori_loop(1, planes, share, 0)
    zall[mz] = zsend[mz]
    pumps(PLAN[4], PLAN[5])

    def shared(i, carry):
        peer = lax.rem(mz + i, planes)
        copy = remote(zsend.at[peer], zall.at[peer], send_z.at[peer], recv_c.at[peer], "mem", peer)
        copy.wait_send()
        copy.wait_recv()
        return carry

    lax.fori_loop(1, planes, shared, 0)

    for c in range(2):
        zpad[:, c, 0:local] = zall[:, c * local : (c + 1) * local]

    row = lax.broadcasted_iota(jnp.int32, (rows, LANES), 0)
    real = (row & 7) < local
    own = pl.ds(pl.multiple_of(mz * LANES, LANES), LANES)
    sd = sd_ref[:, own]
    inverse_scale = 1.0 / (sd * jnp.sqrt(jnp.full(sd.shape, members - 1, F32)))
    gram = jnp.zeros((rows, rows), F32)
    for c in range(2):
        p = zpad[:, c].reshape(rows, LANES)
        mean = jnp.sum(jnp.where(real, p, 0.0), axis=0, keepdims=True) * (1.0 / members)
        anomaly = jnp.where(real, (p - mean) * inverse_scale, 0.0)
        innovation = (obs_ref[c : c + 1, own] - mean) / sd
        left = jnp.where(row == local, innovation, anomaly)
        gram = gram + nt_dot(left, anomaly, HIGHEST)
    chunk = rows // tiles
    for t in range(tiles):
        gsend[t] = gram[chunk * t : chunk * (t + 1)]

    def scatter(i, carry):
        peer = lax.rem(me + i, tiles)
        remote(gsend.at[peer], grecv.at[me], send_a.at[peer], recv_a.at[me], "tile", peer).start()
        return carry

    lax.fori_loop(1, tiles, scatter, 0)
    grecv[me] = gsend[me]
    pumps(PLAN[5], PLAN[6])

    def scattered(i, carry):
        peer = lax.rem(me + i, tiles)
        copy = remote(
            gsend.at[peer], grecv.at[peer], send_a.at[peer], recv_a.at[peer], "tile", peer
        )
        copy.wait_send()
        copy.wait_recv()
        return carry

    lax.fori_loop(1, tiles, scattered, 0)
    partial = grecv[0]
    for t in range(1, tiles):
        partial = partial + grecv[t]
    gpart[...] = partial

    def plane(i, carry):
        peer = lax.rem(mz + i, planes)
        remote(gpart, gplane.at[mz], send_z.at[peer], recv_e.at[mz], "mem", peer).start()
        return carry

    lax.fori_loop(1, planes, plane, 0)
    gplane[mz] = partial
    pumps(PLAN[6], PLAN[7])

    def planed(i, carry):
        peer = lax.rem(mz + i, planes)
        copy = remote(gpart, gplane.at[peer], send_z.at[peer], recv_e.at[peer], "mem", peer)
        copy.wait_send()
        copy.wait_recv()
        return carry

    lax.fori_loop(1, planes, planed, 0)
    summed = gplane[0]
    for z in range(1, planes):
        summed = summed + gplane[z]
    gpart[...] = summed

    def gather(i, carry):
        peer = lax.rem(me + i, tiles)
        remote(gpart, gall.at[me], send_b.at[peer], recv_b.at[me], "tile", peer).start()
        return carry

    lax.fori_loop(1, tiles, gather, 0)
    gall[me] = summed
    pumps(PLAN[7], PLAN[8])

    def gathered(i, carry):
        peer = lax.rem(me + i, tiles)
        copy = remote(gpart, gall.at[peer], send_b.at[peer], recv_b.at[peer], "tile", peer)
        copy.wait_send()
        copy.wait_recv()
        return carry

    lax.fori_loop(1, tiles, gathered, 0)

    for t in range(tiles):
        gfull[chunk * t : chunk * (t + 1), :] = gall[t]
    proj_row = gfull[local : local + 1, :]
    square_row = lax.broadcasted_iota(jnp.int32, (rows, rows), 0)
    square_column = lax.broadcasted_iota(jnp.int32, (rows, rows), 1)
    one = (square_row == square_column).astype(F32)
    left = jnp.where((square_row & 7) < local, gfull[...], 0.0) + one
    inverse = one
    for b in range(planes):
        height = rows - 8 * b
        step_row = lax.broadcasted_iota(jnp.int32, (height, rows), 0)
        for r in range(local):
            k = 8 * b + r
            pivot = left[r : r + 1, k : k + 1]
            scale = lax.rsqrt(pivot)
            scale = scale * (1.5 - 0.5 * pivot * scale * scale)
            left_row = left[r : r + 1] * scale
            inverse_row = inverse[r : r + 1] * scale
            column = jnp.where(step_row > r, left[:, k : k + 1] * scale, 0.0)
            left = left - column * left_row
            inverse = jnp.where(step_row == r, inverse_row, inverse - column * inverse_row)
        weight_t[8 * b : 8 * b + 8, :] = inverse[0:8]
        if b + 1 < planes:
            left, inverse = left[8:], inverse[8:]
        pumps(PLAN[8] + (PLAN[9] - PLAN[8]) * b // planes, PLAN[8] + (PLAN[9] - PLAN[8]) * (b + 1) // planes)

    real_square = ((square_row & 7) < local) & ((square_column & 7) < local)
    root = jnp.where(real_square, weight_t[...], 0.0)
    solved = jnp.sum(root * proj_row, axis=1, keepdims=True)
    mean_weight = jnp.sum(root * solved, axis=0, keepdims=True)
    grown = mean_weight + jnp.sqrt(jnp.full((rows, rows), members - 1, F32)) * root
    grown = jnp.where(real_square, grown, 0.0)
    centre = jnp.sum(grown, axis=1, keepdims=True) * (1.0 / members)
    weights = jnp.where(real_square, grown - centre + 1.0 / members, 0.0)
    weight_t[...] = weights

    for c in range(2):
        share_of = zpad[:, c].reshape(rows, LANES)
        share_of = jnp.where(real, share_of, 0.0)
        moved = jnp.dot(weights, share_of, precision=HIGHEST, preferred_element_type=F32)
        pstage[:, c * local : (c + 1) * local] = moved.reshape(planes, 8, LANES)[:, 0:local]
    psend[...] = pstage[...].astype(BF)

    def give(i, carry):
        peer = lax.rem(mz + i, planes)
        remote(psend.at[peer], pall.at[mz], send_z.at[peer], recv_g.at[mz], "mem", peer).start()
        return carry

    lax.fori_loop(1, planes, give, 0)
    pall[mz] = psend[mz]
    pumps(PLAN[9], PLAN[10])

    own_weights = weight_t[pl.ds(pl.multiple_of(mz * 8, 8), 8), :].astype(BF)
    up_row = lax.broadcasted_iota(jnp.int32, (inner, 8), 0)
    up_column = lax.broadcasted_iota(jnp.int32, (inner, 8), 1)
    tall = jnp.dot(
        ((up_row // layers) == up_column).astype(F32).astype(BF),
        own_weights,
        preferred_element_type=F32,
    ).astype(BF)
    for z in range(planes):
        wide_row = lax.broadcasted_iota(jnp.int32, (rows, 8 * layers), 0)
        wide_column = lax.broadcasted_iota(jnp.int32, (rows, 8 * layers), 1)
        spread = jnp.dot(
            tall,
            (wide_row == 8 * z + wide_column // layers).astype(F32).astype(BF),
            preferred_element_type=F32,
        )
        same = (lax.broadcasted_iota(jnp.int32, (inner, 8 * layers), 0) % layers) == (
            lax.broadcasted_iota(jnp.int32, (inner, 8 * layers), 1) % layers
        )
        kron[z] = jnp.where(same, spread, 0.0).astype(BF)

    def term(source, q):
        block = field[source, q].reshape(inner, piece)
        return jnp.dot(kron[source][:, :inner], block, preferred_element_type=F32)

    def own_term(q, carry):
        acc[q] = term(mz, q)
        return carry

    lax.fori_loop(0, PIECES, own_term, 0)

    def add_slot(n):
        for way in range(2):
            q = lax.rem(n + shift[way], PIECES)
            acc[q] = acc[q] + term(ring_source(way, n), q)

    begin = min(PLAN[10], base - 4)
    rest = base - begin - 1

    def follow(n, carry):
        pump(n)
        j = n - begin

        def late(s, carry):
            add_slot(s)
            return carry

        lax.fori_loop(
            jnp.minimum(j * begin // rest, begin), jnp.minimum((j + 1) * begin // rest, begin), late, 0
        )
        add_slot(n)
        return carry

    lax.fori_loop(begin, base, follow, 0)

    def given(i, carry):
        peer = lax.rem(mz + i, planes)
        copy = remote(psend.at[peer], pall.at[peer], send_z.at[peer], recv_g.at[peer], "mem", peer)
        copy.wait_send()
        copy.wait_recv()
        return carry

    lax.fori_loop(1, planes, given, 0)

    def place(z, carry):
        lanes = pl.ds(pl.multiple_of(z * LANES, LANES), LANES)
        block = pall[z].astype(F32)
        for c in range(2):
            for m in range(local):
                positions_out[m, c : c + 1, lanes] = block[c * local + m : c * local + m + 1]
        return carry

    lax.fori_loop(0, planes, place, 0)

    for n in range(base, max(slots)):
        ways = [way for way in range(2) if n < slots[way]]
        pump(n, ways)
        for way in ways:
            q = (n + shift[way]) % PIECES
            out = acc[q] + term(ring_source(way, n), q)
            velocity_out[:, :, piece * q : piece * (q + 1)] = (
                out.astype(BF).reshape(local, layers, piece)
            )
    for way in range(2):
        for n in range(slots[way] - PIECES, slots[way]):
            ring_out(way, n).wait_send()


def shards(velocity, start_frac, observed, obs_sd, tile_of, cell_of):
    local, comps, levels, cells = velocity.shape
    tiles = lax.axis_size("tile")
    planes = lax.axis_size("mem")
    drifters = cell_of.shape[0]
    layers = comps * levels
    rows = planes * 8
    chunk = rows // tiles
    inner = local * layers
    piece = cells // PIECES
    slots = PIECES * (planes // 2 - 1) + max(UP, PIECES - UP)
    vmem = pl.BlockSpec(memory_space=pltpu.VMEM)
    dma = pltpu.SemaphoreType.DMA
    f32 = lambda *shape: pltpu.VMEM(shape, F32)
    bf16 = lambda *shape: pltpu.VMEM(shape, BF)
    new_velocity, new_positions = pl.pallas_call(
        functools.partial(assimilation_kernel, tiles, planes, local),
        out_shape=(
            jax.ShapeDtypeStruct((local, layers, cells), BF),
            jax.ShapeDtypeStruct((local, comps, drifters), F32),
        ),
        in_specs=[vmem] * 5 + [pl.BlockSpec(memory_space=pltpu.HBM)],
        out_specs=(vmem, vmem),
        scratch_shapes=[
            bf16(planes, PIECES, local, layers, piece),
            bf16(cells // LOW * 16, LOW),
            f32(1, drifters),
            f32(tiles, 8, LANES),
            f32(tiles, 8, LANES),
            f32(tiles, 2, 8, LANES),
            f32(tiles, 2, 8, LANES),
            bf16(tiles * 16, 3 * LANES),
            f32(planes, 2 * local, LANES),
            f32(planes, 2 * local, LANES),
            f32(planes, 2, 8, LANES),
            f32(tiles, chunk, rows),
            f32(tiles, chunk, rows),
            f32(chunk, rows),
            f32(planes, chunk, rows),
            f32(tiles, chunk, rows),
            f32(rows, rows),
            f32(rows, rows),
            bf16(planes, inner, 8 * layers),
            f32(PIECES, inner, piece),
            f32(planes, 2 * local, LANES),
            bf16(planes, 2 * local, LANES),
            bf16(planes, 2 * local, LANES),
            dma((PIECES,)),
            dma((tiles,)),
            dma((tiles,)),
            dma((planes,)),
            dma((tiles,)),
            dma((tiles,)),
            dma((planes,)),
            dma((planes,)),
            dma((planes,)),
            dma((2, PIECES)),
            dma((2, slots)),
        ],
        compiler_params=pltpu.CompilerParams(
            collective_id=0, has_side_effects=True, vmem_limit_bytes=65_700_000
        ),
        name="assimilation",
    )(
        tile_of.reshape(1, drifters),
        cell_of.reshape(1, drifters),
        start_frac,
        observed,
        obs_sd.reshape(1, drifters),
        velocity.reshape(local, layers, cells),
    )
    return (new_velocity.reshape(velocity.shape), new_positions)


def solution(mesh):
    in_specs = (
        P("mem", None, None, "tile"),
        P(None, "tile"),
        P(None, "tile"),
        P("tile"),
        P("tile", None),
        P("tile"),
    )
    out_specs = (P("mem", None, None, "tile"), P("mem", None, "tile"))
    return jax.shard_map(shards, mesh=mesh, in_specs=in_specs, out_specs=out_specs, check_vma=False)
```
